32 devices in a mesh: tm: 4 (over y, x), space: 8 (over z, core).
Axes of the slice: x: 2, y: 2, z: 4, core: 2. Of those that a mesh axis runs over, the one named last changes fastest.
Arguments:
- queries: bfloat16 [4096, 4096], P(('tm', 'space')), may hold values from -20 to 20
- key_vectors: bfloat16 [4096, 4096], P(('tm', 'space')), may hold values from -20 to 20
- value_vectors: bfloat16 [4096, 4096], P(('tm', 'space')), may hold values from -6 to 6
- out_weight: bfloat16 [4096, 6144], P(None, 'space'), may hold values from -0.375 to 0.375
- frame_mask: int32 [4, 4], replicated, may hold values 0 or 1
Outputs:
- projected: bfloat16 [4096, 6144], P('tm', 'space')
The draws below stay inside these ranges and needn't reach their ends.
All inputs are finite; a program needn't handle non-finite values.
Results may differ from the reference program's by a relative error of at most 0.0075.
Values may be sent and summed in bfloat16 or wider, within the bound.
A program may use at most 128 MiB of HBM per device.

```python
import math
import jax
import jax.numpy as jnp
from jax import lax

D = 6144
HD = 128
HEADS = 32
TOK_DEV = 128
WIN = 1
BLOCKS = 4
TOKENS = 4096
N_TM = 4
N_SPACE = 8


def pair_draw(key):
    base = jax.random.fold_in(key, 7193)
    first_key, second_key = jax.random.split(base, 2)
    width = HEADS * HD
    query_draw = 2.0 * jax.random.truncated_normal(first_key, -4.0, 4.0, (TOKENS, width), jnp.float32)
    key_draw = jax.random.truncated_normal(second_key, -4.0, 4.0, (TOKENS, width), jnp.float32)
    return (query_draw, key_draw)


def draw_queries(key, part):
    return pair_draw(key)[0].astype(jnp.bfloat16)


def draw_key_vectors(key, part):
    return pair_draw(key)[1].astype(jnp.bfloat16)


def set_ends(drawn, own_key, least, top_value):
    extent = drawn.shape
    index_at = [jax.random.randint(jax.random.fold_in(own_key, axis), (), 0, extent[axis]) for axis in range(len(extent))]
    drawn = drawn.at[tuple(index_at)].set(least)
    longest = extent.index(max(extent))
    index_at[longest] = (index_at[longest] + 1) % extent[longest]
    return drawn.at[tuple(index_at)].set(top_value)


def block_scale(key, dims, cuts, least, largest):
    gain, own = 1.0, jax.random.fold_in(key, 6)
    for axis_at, blocks in cuts:
        draws = jnp.exp(jax.random.uniform(jax.random.fold_in(own, axis_at), (blocks,), jnp.float32, least / len(cuts), largest / len(cuts)))
        gain = gain * jnp.repeat(draws, dims[axis_at] // blocks).reshape([-1 if axis == axis_at else 1 for axis in range(len(dims))])
    return gain


def noise(key, shape, scale, limit, shards=(), kind=jnp.bfloat16):
    drawn = scale * jax.random.normal(key, shape, jnp.float32)
    if shards:
        drawn = drawn * block_scale(key, shape, shards, -0.22, 0.18)
    return jnp.clip(drawn, -limit, limit).astype(kind)


def setup_inputs(seed: int = 0) -> dict:
    keys = jax.random.split(jax.random.key(seed), 6)
    return {
        "queries": draw_queries(jax.random.fold_in(keys[5], 71), 0),
        "key_vectors": draw_key_vectors(jax.random.fold_in(keys[5], 71), 0),
        "value_vectors": noise(keys[2], (TOKENS, HEADS * HD), 1.0, 6.0, ((0, 32),)),
        "out_weight": noise(keys[3], (HEADS * HD, D), (HEADS * HD // 16) ** -0.5, 0.375, ((1, 8),)),
        "frame_mask": set_ends((jax.random.randint(keys[4], (BLOCKS, BLOCKS), 0, 5) < 4).astype(jnp.int32), jax.random.fold_in(keys[4], 1), 0, 1),
    }


def reference(queries, key_vectors, value_vectors, out_weight, frame_mask):
    block_tokens = TOK_DEV * N_SPACE
    scale_factor = 1.0 / math.sqrt(HD)
    pieces = []
    for frame_index in range(N_TM):
        block_list = [(frame_index + offset) % N_TM for offset in range(-WIN, WIN + 1)]
        query_rows = queries[frame_index * block_tokens:(frame_index + 1) * block_tokens]
        query_rows = query_rows.reshape(block_tokens, HEADS, HD).transpose(1, 0, 2)
        key_rows = jnp.concatenate([key_vectors[b * block_tokens:(b + 1) * block_tokens] for b in block_list], axis=0)
        key_rows = key_rows.reshape(-1, HEADS, HD).transpose(1, 0, 2)
        value_rows = jnp.concatenate([value_vectors[b * block_tokens:(b + 1) * block_tokens] for b in block_list], axis=0)
        value_rows = value_rows.reshape(-1, HEADS, HD).transpose(1, 0, 2)
        owners = jnp.concatenate([jnp.full((block_tokens,), b, jnp.int32) for b in block_list])
        mask_bits = frame_mask[frame_index][owners]
        allowed = (owners == frame_index) | (mask_bits == 1)

        def one_head(head_trio):
            query_head, key_head, value_head = head_trio
            scores = jnp.dot(query_head, key_head.T, preferred_element_type=jnp.float32) * scale_factor
            scores = jnp.where(allowed[None, :], scores, -jnp.inf)
            row_top = lax.optimization_barrier(jnp.max(scores, axis=1, keepdims=True))
            exp_terms = jnp.where(allowed[None, :], jnp.exp(scores - row_top), 0.0)
            totals = lax.optimization_barrier(jnp.sum(exp_terms, axis=1, keepdims=True))
            mixed = jnp.dot(exp_terms.astype(jnp.bfloat16), value_head, preferred_element_type=jnp.float32)
            return mixed / totals
        heads_out = lax.map(one_head, (query_rows, key_rows, value_rows))
        attended = heads_out.transpose(1, 0, 2).reshape(block_tokens, HEADS * HD).astype(jnp.bfloat16)
        pieces.append(jnp.dot(attended, out_weight, preferred_element_type=jnp.float32).astype(jnp.bfloat16))
    return jnp.concatenate(pieces, axis=0)
```

```python
import functools
import math

import jax
import jax.numpy as jnp
from jax import lax
from jax.experimental import pallas as pl
from jax.experimental.pallas import tpu as pltpu
from jax.sharding import PartitionSpec as P

HD = 128
MESH = pl.DeviceIdType.MESH
WINDOW = 2
START = 6.5
STEP = 5.8
LATE = 5.8
HALF = 5.6
HOP = 1.8
TILE = 1.6
IN_HOP = 8.0
OUT_HOP = 8.0
IN_BASE = 84.0
IN_RATE = 1.6
OUT_BASE = 72.0
OUT_RATE = 2.2
KEEP = 2
EARLY = 1.0
RELAY_HOP = 4.0
PROJ = 1.0
SPREAD = 1.8
LAND = 2.0
FINAL = 95.0


def kernel(
    frames, places, heads, pieces,
    q_hbm, k_hbm, v_hbm, w_hbm, mask_ref, out_ref,
    qb, kvb, kvx, kvy, gat, wv, acc,
    a_send, a_recv, x_send, x_recv, y_send, y_recv,
    g_send, m_send, g_recv, p_recv, w_sem,
):
    f = lax.axis_index("tm")
    s = lax.axis_index("space")
    tok = q_hbm.shape[0]
    rows = tok * places
    piece = rows // pieces
    chips = places // 2
    chunks = heads * pieces
    z = lax.div(s, 2)
    core = lax.rem(s, 2)
    odd = lax.rem(f, 2)
    partner = f + 1 - 2 * odd
    onward = lax.rem(f + 2 - 4 * odd + frames, frames)
    behind = lax.rem(f - 2 + 4 * odd + frames, frames)
    far = lax.rem(f - 1 + 2 * odd + frames, frames)
    mate = 2 * z + 1 - core

    def remote(src, dst, send, recv, tm_to, space_to):
        return pltpu.make_async_remote_copy(
            src_ref=src, dst_ref=dst, send_sem=send, recv_sem=recv,
            device_id=(tm_to, space_to), device_id_type=MESH,
        )

    def whole_wait(ref, sem):
        pltpu.make_async_copy(ref, ref, sem).wait()

    barrier = pltpu.get_barrier_semaphore()
    for j in range(1, places):
        pl.semaphore_signal(
            barrier, inc=1, device_id=(f, lax.rem(s + j, places)), device_id_type=MESH
        )
    for other in (partner, onward, behind):
        pl.semaphore_signal(barrier, inc=1, device_id=(other, s), device_id_type=MESH)

    def landing(t, h):
        return qb.at[h] if t == 2 else kvb.at[t, h]

    sources = (k_hbm, v_hbm, q_hbm)
    own_rows = pl.ds(pl.multiple_of(s * tok, tok), tok)

    def head_cols(place, h):
        return pl.ds(pl.multiple_of((place * heads + h) * HD, HD), HD)

    for h in range(heads):
        for t in range(3):
            pltpu.make_async_copy(
                sources[t].at[:, head_cols(s, h)], landing(t, h).at[own_rows, :], a_recv.at[h, t]
            ).start()

    for h in range(heads):
        def load(i, carry):
            pltpu.make_async_copy(
                w_hbm.at[pl.ds(pl.multiple_of((i * heads + h) * HD, HD), HD), :],
                wv.at[h, pl.ds(pl.multiple_of(i * HD, HD), HD), :],
                w_sem.at[h],
            ).start()
            return carry

        lax.fori_loop(0, places, load, 0)

    pl.semaphore_wait(barrier, places - 1 + 3)

    items = [(0, 0), (0, 1)]
    for h in range(1, heads):
        if h < heads - 1 or heads < 3:
            items += [(h, 0), (h - 1, 2), (h, 1)]
        else:
            items += [(h, 0), (h, 1), (h - 1, 2)]
    items.append((heads - 1, 2))
    at_end = (z == 0) | (z == chips - 1)
    lower = 2 * z < chips - 1

    def send_item(i, some=None):
        h, t = items[i]
        for j in range(1, places):
            to = lax.rem(s + j, places)
            away = lax.div(to, 2)
            copy = remote(
                sources[t].at[:, head_cols(to, h)], landing(t, h).at[own_rows, :],
                a_send.at[h, t], a_recv.at[h, t], f, to,
            )
            held = at_end | ((away != z) & ((away < z) == lower))
            if some is None:
                copy.start()
            else:
                pl.when(held if some else jnp.logical_not(held))(copy.start)

    for i in range(len(items)):
        send_item(i, None if i < WINDOW else False)

    def feed(i):
        if i < len(items):
            send_item(i, True)

    def x_copy(h, t):
        return remote(
            kvb.at[t, h], kvx.at[t, h], x_send.at[h, t], x_recv.at[h, t], partner, s
        )

    def y_copy(h, t):
        return remote(
            kvx.at[t, h], kvy.at[t, h], y_send.at[h, t], y_recv.at[h, t], onward, s
        )

    def item_lands(i):
        h, t = items[i]
        whole_wait(landing(t, h), a_recv.at[h, t])
        if t < 2:
            x_copy(h, t).start()
        feed(i + WINDOW)

    def pass_on(h, t):
        x_copy(h, t).wait_recv()
        y_copy(h, t).start()

    def part(c, place):
        return gat.at[c // pieces, place, pl.ds(pl.multiple_of(c % pieces * piece, piece), piece), :]

    def hop(c, origin, slot, to_chip):
        p = part(c, 2 * origin + core)
        return remote(p, p, g_send.at[c, slot], g_recv.at[c, origin], f, 2 * to_chip + core)

    def to_mate(c, origin):
        p = part(c, 2 * origin + core)
        return remote(p, p, m_send.at[c, origin], p_recv.at[c, origin], f, mate)

    def from_mate(c, origin):
        p = part(c, 2 * origin + 1 - core)
        return remote(p, p, m_send.at[c, origin], p_recv.at[c, origin], f, mate)

    def own_hops(c):
        return [(z < chips - 1, hop(c, z, 0, z + 1)), (z > 0, hop(c, z, 1, z - 1))]

    def far_hops(c):
        if chips < 3:
            return []
        return [(z == 0, hop(c, z, 2, z + 2)), (z == chips - 1, hop(c, z, 3, z - 2))]

    def send_own(c):
        for cond, copy in own_hops(c):
            pl.when(cond)(copy.start)
        to_mate(c, z).start()

    def send_far(c):
        for cond, copy in far_hops(c):
            pl.when(cond)(copy.start)

    def passes_on(k, up):
        if up:
            on = (z >= k) & (z < chips - 1)
            return on & (z != 1) if k == 1 else on
        on = (z + k <= chips - 1) & (z > 0)
        return on & (z != chips - 2) if k == 1 else on

    def relay(c, k, edge, more):
        for up in (True, False):
            origin = z - k if up else z + k
            slot = 4 + 2 * (k - 1) + (0 if up else 1)
            here = z >= k if up else z + k <= chips - 1
            here &= (z == k if edge else z != k) if up else (
                z + k == chips - 1 if edge else z + k != chips - 1)
            if k < chips - 1:
                on = passes_on(k, up)
                here &= on if more else jnp.logical_not(on)

            @pl.when(here)
            def _():
                hop(c, origin, slot, z).wait_recv()

            if more:
                @pl.when(here)
                def _():
                    hop(c, origin, slot, z + 1 if up else z - 1).start()

            @pl.when(here)
            def _():
                to_mate(c, origin).start()

    stages = [
        (k, edge, k - 2 if edge and k > 1 else k - 1)
        for k in range(1, chips) for edge in (False, True)
        if edge or k < chips - 1
    ]
    near_pen = jnp.where(mask_ref[f, partner] == 1, 0.0, jnp.inf).astype(jnp.float32)
    far_pen = jnp.where(mask_ref[f, far] == 1, 0.0, jnp.inf).astype(jnp.float32)
    factor = math.log2(math.e) / math.sqrt(HD)

    def attend(h, i):
        at = pl.ds(pl.multiple_of(i * piece, piece), piece)
        q = qb[h, at, :]
        places_kv = ((kvb, None), (kvx, near_pen), (kvy, far_pen))
        scores = []
        top = None
        for ref, pen in places_kv:
            sc = lax.dot_general(
                q, ref[0, h], (((1,), (1,)), ((), ())),
                preferred_element_type=jnp.float32,
            )
            scores.append(sc)
            best = jnp.max(sc, axis=1, keepdims=True)
            best = best if pen is None else best - pen
            top = best if top is None else jnp.maximum(top, best)
        total = None
        mixed = None
        for sc, (ref, pen) in zip(scores, places_kv):
            level = top if pen is None else top + pen
            e = jnp.exp2((sc - level) * factor)
            summed = jnp.sum(e, axis=1, keepdims=True)
            prod = jnp.dot(
                e.astype(jnp.bfloat16), ref[1, h], preferred_element_type=jnp.float32
            )
            total = summed if total is None else total + summed
            mixed = prod if mixed is None else mixed + prod
        gat[h, s, at, :] = (mixed / total).astype(jnp.bfloat16)

    def project(c):
        h = c // pieces
        for o in range(chips):
            from_mate(c, o).wait_recv()
        at = pl.ds(pl.multiple_of(c % pieces * piece, piece), piece)
        a = jnp.concatenate([gat[h, p, at, :] for p in range(places)], axis=1)
        prod = acc[at, :] + jnp.dot(a, wv[h], preferred_element_type=jnp.float32)

        @pl.when(h < heads - 1)
        def _():
            acc[at, :] = prod

        @pl.when(h == heads - 1)
        def _():
            out_ref[at, :] = prod.astype(out_ref.dtype)

    def loop(first, last, fn):
        def step(i, carry):
            fn(i)
            return carry

        if last > first:
            lax.fori_loop(first, last, step, 0)

    acc[...] = jnp.zeros_like(acc)
    scope = jax.named_scope
    events = []
    landed = {}
    x_free = y_free = 0.0
    for i, (h, t) in enumerate(items):
        landed[h, t] = START + STEP * (i + 1) if i < 6 else START + 6 * STEP + LATE * (i - 5)
        events.append((landed[h, t], f"item{i}", functools.partial(item_lands, i)))
        if t < 2:
            x_free = max(x_free, landed[h, t]) + HALF
            events.append((x_free + HOP, f"x{h}{t}", functools.partial(pass_on, h, t)))
            y_free = max(y_free, x_free + HOP) + HALF
            landed[h, t] = y_free + HOP
    now = 0.0
    tile_at = []
    for c in range(chunks):
        now = max([now] + [landed[c // pieces, t] for t in range(3)])
        tile_at.append(now)
        now += TILE
    ends = [0.0] * chunks
    kept = max(heads - KEEP, 0) * pieces
    if kept:
        flush_at = max(tile_at[kept - 1] + TILE, tile_at[kept] - EARLY)
        events.append((flush_at, "flush", lambda: loop(0, kept, send_far)))
    inner_at, outer_at = IN_BASE, OUT_BASE
    for c in range(chunks):
        inner_at = max(inner_at + IN_RATE, tile_at[c] + TILE + IN_HOP)
        outer_at = max(outer_at + OUT_RATE, tile_at[c] + TILE + OUT_HOP)
        for k, edge, depth in stages:
            at = (outer_at if edge else inner_at) + RELAY_HOP * depth
            for more in (True, False):
                if more and k == chips - 1:
                    continue
                when = at if more else max(at + LAND, FINAL + 1.4 * c)
                events.append((when, f"r{k}{int(edge)}{int(more)}_{c}", functools.partial(relay, c, k, edge, more)))
                ends[c] = max(ends[c], when)
    events.sort(key=lambda e: e[0])

    def run(when, fn):
        groups = []
        for c in range(chunks):
            group = []
            while events and events[0][0] <= when[c]:
                group.append(events.pop(0)[1:])
            groups.append(group)

        def step(c):
            for j, group in enumerate(groups):
                if group:
                    @pl.when(c == j)
                    def _():
                        for name, event in group:
                            with scope(name):
                                event()
            fn(c)

        loop(0, chunks, step)

    def tile(c):
        h = c // pieces

        @pl.when(c % pieces == 0)
        def _():
            with scope("ready"):
                for t in range(2):
                    y_copy(h, t).wait_recv()
        with scope("attend"):
            attend(h, c % pieces)
            send_own(c)
            pl.when(c >= kept)(lambda: send_far(c))

    def last(c):
        with scope("project"):
            project(c)

    run(tile_at, tile)
    for h in range(heads):
        whole_wait(wv.at[h], w_sem.at[h])
    run([max(e + PROJ, tile_at[-1] + SPREAD * c) for c, e in enumerate(ends[:-1])] + [math.inf], last)

    for h in range(heads):
        for t in range(3):
            sent = landing(t, h).at[pl.ds(0, (places - 1) * tok), :]
            whole_wait(sent, a_send.at[h, t])
        for t in range(2):
            x_copy(h, t).wait_send()
            y_copy(h, t).wait_send()

    def drain(c):
        for cond, copy in own_hops(c) + far_hops(c):
            pl.when(cond)(copy.wait_send)
        for o in range(chips):
            to_mate(c, o).wait_send()
        for k in range(1, chips - 1):
            for up in (True, False):
                slot = 4 + 2 * (k - 1) + (0 if up else 1)
                origin = z - k if up else z + k

                @pl.when(passes_on(k, up))
                def _():
                    hop(c, origin, slot, z + 1 if up else z - 1).wait_send()

    loop(0, chunks, drain)


def solution(mesh):
    frames = mesh.shape["tm"]
    places = mesh.shape["space"]

    def body(queries, key_vectors, value_vectors, out_weight, frame_mask):
        tok, width = queries.shape
        heads = width // HD // places
        rows = tok * places
        chips = places // 2
        cols = out_weight.shape[1]
        pieces = max(1, rows // 256)
        chunks = heads * pieces
        bf16 = jnp.bfloat16
        anyspace = pl.BlockSpec(memory_space=pl.ANY)
        dma = pltpu.SemaphoreType.DMA
        return pl.pallas_call(
            functools.partial(kernel, frames, places, heads, pieces),
            out_shape=jax.ShapeDtypeStruct((rows, cols), bf16),
            in_specs=[anyspace] * 4 + [pl.BlockSpec(memory_space=pltpu.SMEM)],
            out_specs=pl.BlockSpec(memory_space=pltpu.VMEM),
            scratch_shapes=[
                pltpu.VMEM((heads, rows, HD), bf16),
                pltpu.VMEM((2, heads, rows, HD), bf16),
                pltpu.VMEM((2, heads, rows, HD), bf16),
                pltpu.VMEM((2, heads, rows, HD), bf16),
                pltpu.VMEM((heads, places, rows, HD), bf16),
                pltpu.VMEM((heads, places * HD, cols), bf16),
                pltpu.VMEM((rows, cols), jnp.float32),
                dma((heads, 3)), dma((heads, 3)),
                dma((heads, 2)), dma((heads, 2)),
                dma((heads, 2)), dma((heads, 2)),
                dma((chunks, 4 + 2 * (chips - 1))),
                dma((chunks, chips)),
                dma((chunks, chips)),
                dma((chunks, chips)),
                dma((heads,)),
            ],
            compiler_params=pltpu.CompilerParams(
                collective_id=0, has_side_effects=True,
                vmem_limit_bytes=60 * 1024 * 1024,
            ),
        )(queries, key_vectors, value_vectors, out_weight, frame_mask)

    in_specs = (
        P(("tm", "space"), None),
        P(("tm", "space"), None),
        P(("tm", "space"), None),
        P(None, "space"),
        P(),
    )
    return jax.shard_map(
        body, mesh=mesh, in_specs=in_specs, out_specs=P("tm", "space"), check_vma=False
    )
```

```python
import functools
import math

import jax
import jax.numpy as jnp
from jax import lax
from jax.experimental import pallas as pl
from jax.experimental.pallas import tpu as pltpu
from jax.sharding import PartitionSpec as P

HD = 128
MESH = pl.DeviceIdType.MESH
WINDOW = 2
WINDOW_OUT = 6
START = 6.5
STEP = 5.8
LATE = 5.8
HALF = 5.6
HOP = 1.8
TILE = 1.6
IN_HOP = 8.0
OUT_HOP = 8.0
IN_BASE = 84.0
IN_RATE = 1.6
OUT_BASE = 72.0
OUT_RATE = 2.2
KEEP = 2
EARLY = 1.0
RELAY_HOP = 4.0
PROJ = 1.0
DRAIN = 4
SPREAD = 1.8
LAND = 2.0
FINAL = 95.0


def kernel(
    frames, places, heads, pieces,
    q_hbm, k_hbm, v_hbm, w_hbm, mask_ref, out_ref,
    qb, kvb, kvx, kvy, gat, wv, acc,
    a_send, a_recv, x_send, x_recv, y_send, y_recv,
    g_send, m_send, g_recv, p_recv, w_sem,
):
    f = lax.axis_index("tm")
    s = lax.axis_index("space")
    tok = q_hbm.shape[0]
    rows = tok * places
    piece = rows // pieces
    chips = places // 2
    chunks = heads * pieces
    z = lax.div(s, 2)
    core = lax.rem(s, 2)
    odd = lax.rem(f, 2)
    partner = f + 1 - 2 * odd
    onward = lax.rem(f + 2 - 4 * odd + frames, frames)
    behind = lax.rem(f - 2 + 4 * odd + frames, frames)
    far = lax.rem(f - 1 + 2 * odd + frames, frames)
    mate = 2 * z + 1 - core

    def remote(src, dst, send, recv, tm_to, space_to):
        return pltpu.make_async_remote_copy(
            src_ref=src, dst_ref=dst, send_sem=send, recv_sem=recv,
            device_id=(tm_to, space_to), device_id_type=MESH,
        )

    def whole_wait(ref, sem):
        pltpu.make_async_copy(ref, ref, sem).wait()

    barrier = pltpu.get_barrier_semaphore()
    for j in range(1, places):
        pl.semaphore_signal(
            barrier, inc=1, device_id=(f, lax.rem(s + j, places)), device_id_type=MESH
        )
    for other in (partner, onward, behind):
        pl.semaphore_signal(barrier, inc=1, device_id=(other, s), device_id_type=MESH)

    def landing(t, h):
        return qb.at[h] if t == 2 else kvb.at[t, h]

    sources = (k_hbm, v_hbm, q_hbm)
    own_rows = pl.ds(pl.multiple_of(s * tok, tok), tok)

    def head_cols(place, h):
        return pl.ds(pl.multiple_of((place * heads + h) * HD, HD), HD)

    for h in range(heads):
        for t in range(3):
            pltpu.make_async_copy(
                sources[t].at[:, head_cols(s, h)], landing(t, h).at[own_rows, :], a_recv.at[h, t]
            ).start()

    for h in range(heads):
        def load(i, carry):
            pltpu.make_async_copy(
                w_hbm.at[pl.ds(pl.multiple_of((i * heads + h) * HD, HD), HD), :],
                wv.at[h, pl.ds(pl.multiple_of(i * HD, HD), HD), :],
                w_sem.at[h],
            ).start()
            return carry

        lax.fori_loop(0, places, load, 0)

    pl.semaphore_wait(barrier, places - 1 + 3)

    items = [(0, 0), (0, 1)]
    for h in range(1, heads):
        if h < heads - 1 or heads < 3:
            items += [(h, 0), (h - 1, 2), (h, 1)]
        else:
            items += [(h, 0), (h, 1), (h - 1, 2)]
    items.append((heads - 1, 2))
    at_end = (z == 0) | (z == chips - 1)
    lower = 2 * z < chips - 1

    def send_item(i, kinds):
        h, t = items[i]
        for j in range(1, places):
            to = lax.rem(s + j, places)
            away = lax.div(to, 2)
            copy = remote(
                sources[t].at[:, head_cols(to, h)], landing(t, h).at[own_rows, :],
                a_send.at[h, t], a_recv.at[h, t], f, to,
            )
            outward = (away != z) & ((away < z) == lower)
            masks = (jnp.logical_not(at_end | outward), at_end, jnp.logical_not(at_end) & outward)
            go = [m for m, wanted in zip(masks, kinds) if wanted]
            if len(go) == len(masks):
                copy.start()
            elif go:
                pl.when(functools.reduce(jnp.logical_or, go))(copy.start)

    for i in range(len(items)):
        send_item(i, (True, i < WINDOW, i < WINDOW_OUT))

    def feed(i):
        for j, kinds in ((i + WINDOW, (False, True, False)), (i + WINDOW_OUT, (False, False, True))):
            if j < len(items):
                send_item(j, kinds)

    def x_copy(h, t):
        return remote(
            kvb.at[t, h], kvx.at[t, h], x_send.at[h, t], x_recv.at[h, t], partner, s
        )

    def y_copy(h, t):
        return remote(
            kvx.at[t, h], kvy.at[t, h], y_send.at[h, t], y_recv.at[h, t], onward, s
        )

    def item_lands(i):
        h, t = items[i]
        whole_wait(landing(t, h), a_recv.at[h, t])
        if t < 2:
            x_copy(h, t).start()
        feed(i)

    def pass_on(h, t):
        x_copy(h, t).wait_recv()
        y_copy(h, t).start()

    def part(c, place):
        return gat.at[c // pieces, place, pl.ds(pl.multiple_of(c % pieces * piece, piece), piece), :]

    def hop(c, origin, slot, to_chip):
        p = part(c, 2 * origin + core)
        return remote(p, p, g_send.at[c, slot], g_recv.at[c, origin], f, 2 * to_chip + core)

    def to_mate(c, origin):
        p = part(c, 2 * origin + core)
        return remote(p, p, m_send.at[c, origin], p_recv.at[c, origin], f, mate)

    def from_mate(c, origin):
        p = part(c, 2 * origin + 1 - core)
        return remote(p, p, m_send.at[c, origin], p_recv.at[c, origin], f, mate)

    def own_hops(c):
        return [(z < chips - 1, hop(c, z, 0, z + 1)), (z > 0, hop(c, z, 1, z - 1))]

    def far_hops(c):
        if chips < 3:
            return []
        return [(z == 0, hop(c, z, 2, z + 2)), (z == chips - 1, hop(c, z, 3, z - 2))]

    def send_own(c):
        for cond, copy in own_hops(c):
            pl.when(cond)(copy.start)
        to_mate(c, z).start()

    def send_far(c):
        for cond, copy in far_hops(c):
            pl.when(cond)(copy.start)

    def passes_on(k, up):
        if up:
            on = (z >= k) & (z < chips - 1)
            return on & (z != 1) if k == 1 else on
        on = (z + k <= chips - 1) & (z > 0)
        return on & (z != chips - 2) if k == 1 else on

    def relay(c, k, edge, more):
        for up in (True, False):
            origin = z - k if up else z + k
            slot = 4 + 2 * (k - 1) + (0 if up else 1)
            here = z >= k if up else z + k <= chips - 1
            here &= (z == k if edge else z != k) if up else (
                z + k == chips - 1 if edge else z + k != chips - 1)
            if k < chips - 1:
                on = passes_on(k, up)
                here &= on if more else jnp.logical_not(on)

            @pl.when(here)
            def _():
                hop(c, origin, slot, z).wait_recv()

            if more:
                @pl.when(here)
                def _():
                    hop(c, origin, slot, z + 1 if up else z - 1).start()

            @pl.when(here)
            def _():
                to_mate(c, origin).start()

    stages = [
        (k, edge, k - 2 if edge and k > 1 else k - 1)
        for k in range(1, chips) for edge in (False, True)
        if edge or k < chips - 1
    ]
    near_pen = jnp.where(mask_ref[f, partner] == 1, 0.0, jnp.inf).astype(jnp.float32)
    far_pen = jnp.where(mask_ref[f, far] == 1, 0.0, jnp.inf).astype(jnp.float32)
    factor = math.log2(math.e) / math.sqrt(HD)

    def attend(h, i):
        at = pl.ds(pl.multiple_of(i * piece, piece), piece)
        q = qb[h, at, :]
        places_kv = ((kvb, None), (kvx, near_pen), (kvy, far_pen))
        scores = []
        top = None
        for ref, pen in places_kv:
            sc = lax.dot_general(
                q, ref[0, h], (((1,), (1,)), ((), ())),
                preferred_element_type=jnp.float32,
            )
            scores.append(sc)
            best = jnp.max(sc, axis=1, keepdims=True)
            best = best if pen is None else best - pen
            top = best if top is None else jnp.maximum(top, best)
        total = None
        mixed = None
        for sc, (ref, pen) in zip(scores, places_kv):
            level = top if pen is None else top + pen
            e = jnp.exp2((sc - level) * factor)
            summed = jnp.sum(e, axis=1, keepdims=True)
            prod = jnp.dot(
                e.astype(jnp.bfloat16), ref[1, h], preferred_element_type=jnp.float32
            )
            total = summed if total is None else total + summed
            mixed = prod if mixed is None else mixed + prod
        gat[h, s, at, :] = (mixed / total).astype(jnp.bfloat16)

    def project(c):
        h = c // pieces
        for o in range(chips):
            from_mate(c, o).wait_recv()
        at = pl.ds(pl.multiple_of(c % pieces * piece, piece), piece)
        a = jnp.concatenate([gat[h, p, at, :] for p in range(places)], axis=1)
        prod = acc[at, :] + jnp.dot(a, wv[h], preferred_element_type=jnp.float32)

        @pl.when(h < heads - 1)
        def _():
            acc[at, :] = prod

        @pl.when(h == heads - 1)
        def _():
            out_ref[at, :] = prod.astype(out_ref.dtype)

    def loop(first, last, fn):
        def step(i, carry):
            fn(i)
            return carry

        if last > first:
            lax.fori_loop(first, last, step, 0)

    def drain(c):
        for cond, copy in own_hops(c) + far_hops(c):
            pl.when(cond)(copy.wait_send)
        for o in range(chips):
            to_mate(c, o).wait_send()
        for k in range(1, chips - 1):
            for up in (True, False):
                slot = 4 + 2 * (k - 1) + (0 if up else 1)
                origin = z - k if up else z + k

                @pl.when(passes_on(k, up))
                def _():
                    hop(c, origin, slot, z + 1 if up else z - 1).wait_send()

    acc[...] = jnp.zeros_like(acc)
    scope = jax.named_scope
    events = []
    landed = {}
    x_free = y_free = 0.0
    for i, (h, t) in enumerate(items):
        landed[h, t] = START + STEP * (i + 1) if i < 6 else START + 6 * STEP + LATE * (i - 5)
        events.append((landed[h, t], f"item{i}", functools.partial(item_lands, i)))
        if t < 2:
            x_free = max(x_free, landed[h, t]) + HALF
            events.append((x_free + HOP, f"x{h}{t}", functools.partial(pass_on, h, t)))
            y_free = max(y_free, x_free + HOP) + HALF
            landed[h, t] = y_free + HOP
    now = 0.0
    tile_at = []
    for c in range(chunks):
        now = max([now] + [landed[c // pieces, t] for t in range(3)])
        tile_at.append(now)
        now += TILE
    ends = [0.0] * chunks
    kept = max(heads - KEEP, 0) * pieces
    if kept:
        flush_at = max(tile_at[kept - 1] + TILE, tile_at[kept] - EARLY)
        events.append((flush_at, "flush", lambda: loop(0, kept, send_far)))
    inner_at, outer_at = IN_BASE, OUT_BASE
    for c in range(chunks):
        inner_at = max(inner_at + IN_RATE, tile_at[c] + TILE + IN_HOP)
        outer_at = max(outer_at + OUT_RATE, tile_at[c] + TILE + OUT_HOP)
        for k, edge, depth in stages:
            at = (outer_at if edge else inner_at) + RELAY_HOP * depth
            for more in (True, False):
                if more and k == chips - 1:
                    continue
                when = at if more else max(at + LAND, FINAL + 1.4 * c)
                events.append((when, f"r{k}{int(edge)}{int(more)}_{c}", functools.partial(relay, c, k, edge, more)))
                ends[c] = max(ends[c], when)
    events.sort(key=lambda e: e[0])

    def run(when, fn):
        groups = []
        for c in range(chunks):
            group = []
            while events and events[0][0] <= when[c]:
                group.append(events.pop(0)[1:])
            groups.append(group)

        def step(c):
            for j, group in enumerate(groups):
                if group:
                    @pl.when(c == j)
                    def _():
                        for name, event in group:
                            with scope(name):
                                event()
            fn(c)

        loop(0, chunks, step)

    def tile(c):
        h = c // pieces

        @pl.when(c % pieces == 0)
        def _():
            with scope("ready"):
                for t in range(2):
                    y_copy(h, t).wait_recv()
        with scope("attend"):
            attend(h, c % pieces)
            send_own(c)
            pl.when(c >= kept)(lambda: send_far(c))

    def last(c):
        with scope("project"):
            project(c)
        pl.when(c >= DRAIN)(lambda: drain(c - DRAIN))

    run(tile_at, tile)
    for h in range(heads):
        for t in range(3):
            sent = landing(t, h).at[pl.ds(0, (places - 1) * tok), :]
            whole_wait(sent, a_send.at[h, t])
        for t in range(2):
            x_copy(h, t).wait_send()
            y_copy(h, t).wait_send()
    for h in range(heads):
        whole_wait(wv.at[h], w_sem.at[h])
    run([max(e + PROJ, tile_at[-1] + SPREAD * c) for c, e in enumerate(ends[:-1])] + [math.inf], last)

    loop(max(chunks - DRAIN, 0), chunks, drain)


def solution(mesh):
    frames = mesh.shape["tm"]
    places = mesh.shape["space"]

    def body(queries, key_vectors, value_vectors, out_weight, frame_mask):
        tok, width = queries.shape
        heads = width // HD // places
        rows = tok * places
        chips = places // 2
        cols = out_weight.shape[1]
        pieces = max(1, rows // 256)
        chunks = heads * pieces
        bf16 = jnp.bfloat16
        anyspace = pl.BlockSpec(memory_space=pl.ANY)
        dma = pltpu.SemaphoreType.DMA
        return pl.pallas_call(
            functools.partial(kernel, frames, places, heads, pieces),
            out_shape=pltpu.VMEM((rows, cols), bf16),
            in_specs=[anyspace] * 4 + [pl.BlockSpec(memory_space=pltpu.SMEM)],
            out_specs=pl.BlockSpec(memory_space=pltpu.VMEM),
            scratch_shapes=[
                pltpu.VMEM((heads, rows, HD), bf16),
                pltpu.VMEM((2, heads, rows, HD), bf16),
                pltpu.VMEM((2, heads, rows, HD), bf16),
                pltpu.VMEM((2, heads, rows, HD), bf16),
                pltpu.VMEM((heads, places, rows, HD), bf16),
                pltpu.VMEM((heads, places * HD, cols), bf16),
                pltpu.VMEM((rows, cols), jnp.float32),
                dma((heads, 3)), dma((heads, 3)),
                dma((heads, 2)), dma((heads, 2)),
                dma((heads, 2)), dma((heads, 2)),
                dma((chunks, 4 + 2 * (chips - 1))),
                dma((chunks, chips)),
                dma((chunks, chips)),
                dma((chunks, chips)),
                dma((heads,)),
            ],
            compiler_params=pltpu.CompilerParams(
                collective_id=0, has_side_effects=True,
                vmem_limit_bytes=60 * 1024 * 1024,
            ),
        )(queries, key_vectors, value_vectors, out_weight, frame_mask)

    in_specs = (
        P(("tm", "space"), None),
        P(("tm", "space"), None),
        P(("tm", "space"), None),
        P(None, "space"),
        P(),
    )
    return jax.shard_map(
        body, mesh=mesh, in_specs=in_specs, out_specs=P("tm", "space"), check_vma=False
    )
```

```python
import functools
import math

import jax
import jax.numpy as jnp
from jax import lax
from jax.experimental import pallas as pl
from jax.experimental.pallas import tpu as pltpu
from jax.sharding import PartitionSpec as P

HD = 128
MESH = pl.DeviceIdType.MESH
WINDOW = 2
WINDOW_OUT = 3
START = 6.5
STEP = 5.8
LATE = 5.8
LAST = 4.0
HALF = 5.6
HOP = 1.8
TILE = 1.6
IN_HOP = 8.0
OUT_HOP = 8.0
IN_BASE = 84.0
IN_RATE = 1.6
OUT_BASE = 74.0
OUT_RATE = 2.2
KEEP = 2
EARLY = 1.0
RELAY_HOP = 4.0
PROJ = 1.0
DRAIN = 4
SPREAD = 1.8
LAND = 2.0
FINAL = 88.0


def kernel(
    frames, places, heads, pieces,
    q_hbm, k_hbm, v_hbm, w_hbm, mask_ref, out_ref,
    qb, kvb, kvx, kvy, gat, wv, acc,
    a_send, a_recv, x_send, x_recv, y_send, y_recv,
    g_send, m_send, g_recv, p_recv, w_sem,
):
    f = lax.axis_index("tm")
    s = lax.axis_index("space")
    tok = q_hbm.shape[0]
    rows = tok * places
    piece = rows // pieces
    chips = places // 2
    chunks = heads * pieces
    z = lax.div(s, 2)
    core = lax.rem(s, 2)
    odd = lax.rem(f, 2)
    partner = f + 1 - 2 * odd
    onward = lax.rem(f + 2 - 4 * odd + frames, frames)
    behind = lax.rem(f - 2 + 4 * odd + frames, frames)
    far = lax.rem(f - 1 + 2 * odd + frames, frames)
    mate = 2 * z + 1 - core

    def remote(src, dst, send, recv, tm_to, space_to):
        return pltpu.make_async_remote_copy(
            src_ref=src, dst_ref=dst, send_sem=send, recv_sem=recv,
            device_id=(tm_to, space_to), device_id_type=MESH,
        )

    def whole_wait(ref, sem):
        pltpu.make_async_copy(ref, ref, sem).wait()

    barrier = pltpu.get_barrier_semaphore()
    for j in range(1, places):
        pl.semaphore_signal(
            barrier, inc=1, device_id=(f, lax.rem(s + j, places)), device_id_type=MESH
        )
    for other in (partner, onward, behind):
        pl.semaphore_signal(barrier, inc=1, device_id=(other, s), device_id_type=MESH)

    def landing(t, h):
        return qb.at[h] if t == 2 else kvb.at[t, h]

    sources = (k_hbm, v_hbm, q_hbm)
    own_rows = pl.ds(pl.multiple_of(s * tok, tok), tok)

    def head_cols(place, h):
        return pl.ds(pl.multiple_of((place * heads + h) * HD, HD), HD)

    for h in range(heads):
        for t in range(3):
            pltpu.make_async_copy(
                sources[t].at[:, head_cols(s, h)], landing(t, h).at[own_rows, :], a_recv.at[h, t]
            ).start()

    for h in range(heads):
        def load(i, carry):
            pltpu.make_async_copy(
                w_hbm.at[pl.ds(pl.multiple_of((i * heads + h) * HD, HD), HD), :],
                wv.at[h, pl.ds(pl.multiple_of(i * HD, HD), HD), :],
                w_sem.at[h],
            ).start()
            return carry

        lax.fori_loop(0, places, load, 0)

    pl.semaphore_wait(barrier, places - 1 + 3)

    items = [(0, 0), (0, 1)]
    for h in range(1, heads):
        if h < heads - 1 or heads < 3:
            items += [(h, 0), (h - 1, 2), (h, 1)]
        else:
            items += [(h, 0), (h, 1), (h - 1, 2)]
    items.append((heads - 1, 2))
    at_end = (z == 0) | (z == chips - 1)
    lower = 2 * z < chips - 1

    def send_item(i, kinds):
        h, t = items[i]
        for j in range(1, places):
            to = lax.rem(s + j, places)
            away = lax.div(to, 2)
            copy = remote(
                sources[t].at[:, head_cols(to, h)], landing(t, h).at[own_rows, :],
                a_send.at[h, t], a_recv.at[h, t], f, to,
            )
            outward = (away != z) & ((away < z) == lower)
            masks = (jnp.logical_not(at_end | outward), at_end, jnp.logical_not(at_end) & outward)
            go = [m for m, wanted in zip(masks, kinds) if wanted]
            if len(go) == len(masks):
                copy.start()
            elif go:
                pl.when(functools.reduce(jnp.logical_or, go))(copy.start)

    for i in range(len(items)):
        send_item(i, (True, i < WINDOW, i < WINDOW_OUT))

    def feed(i):
        for j, kinds in ((i + WINDOW, (False, True, False)), (i + WINDOW_OUT, (False, False, True))):
            if j < len(items):
                send_item(j, kinds)

    def x_copy(h, t):
        return remote(
            kvb.at[t, h], kvx.at[t, h], x_send.at[h, t], x_recv.at[h, t], partner, s
        )

    def y_copy(h, t):
        return remote(
            kvx.at[t, h], kvy.at[t, h], y_send.at[h, t], y_recv.at[h, t], onward, s
        )

    def item_lands(i):
        h, t = items[i]
        whole_wait(landing(t, h), a_recv.at[h, t])
        if t < 2:
            x_copy(h, t).start()
        feed(i)

    def pass_on(h, t):
        x_copy(h, t).wait_recv()
        y_copy(h, t).start()

    def part(c, place):
        return gat.at[c // pieces, place, pl.ds(pl.multiple_of(c % pieces * piece, piece), piece), :]

    def hop(c, origin, slot, to_chip):
        p = part(c, 2 * origin + core)
        return remote(p, p, g_send.at[c, slot], g_recv.at[c, origin], f, 2 * to_chip + core)

    def to_mate(c, origin):
        p = part(c, 2 * origin + core)
        return remote(p, p, m_send.at[c, origin], p_recv.at[c, origin], f, mate)

    def from_mate(c, origin):
        p = part(c, 2 * origin + 1 - core)
        return remote(p, p, m_send.at[c, origin], p_recv.at[c, origin], f, mate)

    def own_hops(c):
        return [(z < chips - 1, hop(c, z, 0, z + 1)), (z > 0, hop(c, z, 1, z - 1))]

    def far_hops(c):
        if chips < 3:
            return []
        return [(z == 0, hop(c, z, 2, z + 2)), (z == chips - 1, hop(c, z, 3, z - 2))]

    def send_own(c):
        for cond, copy in own_hops(c):
            pl.when(cond)(copy.start)
        to_mate(c, z).start()

    def send_far(c):
        for cond, copy in far_hops(c):
            pl.when(cond)(copy.start)

    def passes_on(k, up):
        if up:
            on = (z >= k) & (z < chips - 1)
            return on & (z != 1) if k == 1 else on
        on = (z + k <= chips - 1) & (z > 0)
        return on & (z != chips - 2) if k == 1 else on

    def relay(c, k, edge, more):
        for up in (True, False):
            origin = z - k if up else z + k
            slot = 4 + 2 * (k - 1) + (0 if up else 1)
            here = z >= k if up else z + k <= chips - 1
            here &= (z == k if edge else z != k) if up else (
                z + k == chips - 1 if edge else z + k != chips - 1)
            if k < chips - 1:
                on = passes_on(k, up)
                here &= on if more else jnp.logical_not(on)

            @pl.when(here)
            def _():
                hop(c, origin, slot, z).wait_recv()

            if more:
                @pl.when(here)
                def _():
                    hop(c, origin, slot, z + 1 if up else z - 1).start()

            @pl.when(here)
            def _():
                to_mate(c, origin).start()

    stages = [
        (k, edge, k - 2 if edge and k > 1 else k - 1)
        for k in range(1, chips) for edge in (False, True)
        if edge or k < chips - 1
    ]
    near_pen = jnp.where(mask_ref[f, partner] == 1, 0.0, jnp.inf).astype(jnp.float32)
    far_pen = jnp.where(mask_ref[f, far] == 1, 0.0, jnp.inf).astype(jnp.float32)
    factor = math.log2(math.e) / math.sqrt(HD)

    def attend(h, i):
        at = pl.ds(pl.multiple_of(i * piece, piece), piece)
        q = qb[h, at, :]
        places_kv = ((kvb, None), (kvx, near_pen), (kvy, far_pen))
        scores = []
        top = None
        for ref, pen in places_kv:
            sc = lax.dot_general(
                q, ref[0, h], (((1,), (1,)), ((), ())),
                preferred_element_type=jnp.float32,
            )
            scores.append(sc)
            best = jnp.max(sc, axis=1, keepdims=True)
            best = best if pen is None else best - pen
            top = best if top is None else jnp.maximum(top, best)
        total = None
        mixed = None
        for sc, (ref, pen) in zip(scores, places_kv):
            level = top if pen is None else top + pen
            e = jnp.exp2((sc - level) * factor)
            summed = jnp.sum(e, axis=1, keepdims=True)
            prod = jnp.dot(
                e.astype(jnp.bfloat16), ref[1, h], preferred_element_type=jnp.float32
            )
            total = summed if total is None else total + summed
            mixed = prod if mixed is None else mixed + prod
        gat[h, s, at, :] = (mixed / total).astype(jnp.bfloat16)

    def project(c):
        h = c // pieces
        for o in range(chips):
            from_mate(c, o).wait_recv()
        at = pl.ds(pl.multiple_of(c % pieces * piece, piece), piece)
        a = jnp.concatenate([gat[h, p, at, :] for p in range(places)], axis=1)
        prod = acc[at, :] + jnp.dot(a, wv[h], preferred_element_type=jnp.float32)

        @pl.when(h < heads - 1)
        def _():
            acc[at, :] = prod

        @pl.when(h == heads - 1)
        def _():
            out_ref[at, :] = prod.astype(out_ref.dtype)

    def loop(first, last, fn):
        def step(i, carry):
            fn(i)
            return carry

        if last > first:
            lax.fori_loop(first, last, step, 0)

    def drain(c):
        for cond, copy in own_hops(c) + far_hops(c):
            pl.when(cond)(copy.wait_send)
        for o in range(chips):
            to_mate(c, o).wait_send()
        for k in range(1, chips - 1):
            for up in (True, False):
                slot = 4 + 2 * (k - 1) + (0 if up else 1)
                origin = z - k if up else z + k

                @pl.when(passes_on(k, up))
                def _():
                    hop(c, origin, slot, z + 1 if up else z - 1).wait_send()

    acc[...] = jnp.zeros_like(acc)
    scope = jax.named_scope
    events = []
    landed = {}
    x_free = y_free = 0.0
    for i, (h, t) in enumerate(items):
        landed[h, t] = START + STEP * (i + 1) if i < 6 else START + 6 * STEP + LATE * (i - 5)
        if i == len(items) - 1:
            landed[h, t] += LAST
        events.append((landed[h, t], f"item{i}", functools.partial(item_lands, i)))
        if t < 2:
            x_free = max(x_free, landed[h, t]) + HALF
            events.append((x_free + HOP, f"x{h}{t}", functools.partial(pass_on, h, t)))
            y_free = max(y_free, x_free + HOP) + HALF
            landed[h, t] = y_free + HOP
    now = 0.0
    tile_at = []
    for c in range(chunks):
        now = max([now] + [landed[c // pieces, t] for t in range(3)])
        tile_at.append(now)
        now += TILE
    ends = [0.0] * chunks
    kept = max(heads - KEEP, 0) * pieces
    if kept:
        flush_at = max(tile_at[kept - 1] + TILE, tile_at[kept] - EARLY)
        events.append((flush_at, "flush", lambda: loop(0, kept, send_far)))
    inner_at, outer_at = IN_BASE, OUT_BASE
    for c in range(chunks):
        inner_at = max(inner_at + IN_RATE, tile_at[c] + TILE + IN_HOP)
        outer_at = max(outer_at + OUT_RATE, tile_at[c] + TILE + OUT_HOP)
        for k, edge, depth in stages:
            at = (outer_at if edge else inner_at) + RELAY_HOP * depth
            for more in (True, False):
                if more and k == chips - 1:
                    continue
                when = at if more else max(at + LAND, FINAL + 1.4 * c)
                events.append((when, f"r{k}{int(edge)}{int(more)}_{c}", functools.partial(relay, c, k, edge, more)))
                ends[c] = max(ends[c], when)
    events.sort(key=lambda e: e[0])

    def run(when, fn):
        groups = []
        for c in range(chunks):
            group = []
            while events and events[0][0] <= when[c]:
                group.append(events.pop(0)[1:])
            groups.append(group)

        def step(c):
            for j, group in enumerate(groups):
                if group:
                    @pl.when(c == j)
                    def _():
                        for name, event in group:
                            with scope(name):
                                event()
            fn(c)

        loop(0, chunks, step)

    def tile(c):
        h = c // pieces

        @pl.when(c % pieces == 0)
        def _():
            with scope("ready"):
                for t in range(2):
                    y_copy(h, t).wait_recv()
        with scope("attend"):
            attend(h, c % pieces)
            send_own(c)
            pl.when(c >= kept)(lambda: send_far(c))

    def last(c):
        with scope("project"):
            project(c)
        pl.when(c >= DRAIN)(lambda: drain(c - DRAIN))

    run(tile_at, tile)
    for h in range(heads):
        for t in range(3):
            sent = landing(t, h).at[pl.ds(0, (places - 1) * tok), :]
            whole_wait(sent, a_send.at[h, t])
        for t in range(2):
            x_copy(h, t).wait_send()
            y_copy(h, t).wait_send()
    for h in range(heads):
        whole_wait(wv.at[h], w_sem.at[h])
    run([max(e + PROJ, tile_at[-1] + SPREAD * c) for c, e in enumerate(ends[:-1])] + [math.inf], last)

    loop(max(chunks - DRAIN, 0), chunks, drain)


def solution(mesh):
    frames = mesh.shape["tm"]
    places = mesh.shape["space"]

    def body(queries, key_vectors, value_vectors, out_weight, frame_mask):
        tok, width = queries.shape
        heads = width // HD // places
        rows = tok * places
        chips = places // 2
        cols = out_weight.shape[1]
        pieces = max(1, rows // 256)
        chunks = heads * pieces
        bf16 = jnp.bfloat16
        anyspace = pl.BlockSpec(memory_space=pl.ANY)
        dma = pltpu.SemaphoreType.DMA
        return pl.pallas_call(
            functools.partial(kernel, frames, places, heads, pieces),
            out_shape=pltpu.VMEM((rows, cols), bf16),
            in_specs=[anyspace] * 4 + [pl.BlockSpec(memory_space=pltpu.SMEM)],
            out_specs=pl.BlockSpec(memory_space=pltpu.VMEM),
            scratch_shapes=[
                pltpu.VMEM((heads, rows, HD), bf16),
                pltpu.VMEM((2, heads, rows, HD), bf16),
                pltpu.VMEM((2, heads, rows, HD), bf16),
                pltpu.VMEM((2, heads, rows, HD), bf16),
                pltpu.VMEM((heads, places, rows, HD), bf16),
                pltpu.VMEM((heads, places * HD, cols), bf16),
                pltpu.VMEM((rows, cols), jnp.float32),
                dma((heads, 3)), dma((heads, 3)),
                dma((heads, 2)), dma((heads, 2)),
                dma((heads, 2)), dma((heads, 2)),
                dma((chunks, 4 + 2 * (chips - 1))),
                dma((chunks, chips)),
                dma((chunks, chips)),
                dma((chunks, chips)),
                dma((heads,)),
            ],
            compiler_params=pltpu.CompilerParams(
                collective_id=0, has_side_effects=True,
                vmem_limit_bytes=60 * 1024 * 1024,
            ),
        )(queries, key_vectors, value_vectors, out_weight, frame_mask)

    in_specs = (
        P(("tm", "space"), None),
        P(("tm", "space"), None),
        P(("tm", "space"), None),
        P(None, "space"),
        P(),
    )
    return jax.shard_map(
        body, mesh=mesh, in_specs=in_specs, out_specs=P("tm", "space"), check_vma=False
    )
```
